32 devices in a mesh: rep: 4 (over x, y), pp: 8 (over z, core).
Axes of the slice: x: 2, y: 2, z: 4, core: 2. Of those that a mesh axis runs over, the one named last changes fastest.
Arguments:
- x: bfloat16 [64, 512, 512], P('rep'), parts along dimension 0
- dy: bfloat16 [64, 512, 512], P('rep'), parts along dimension 0
- w_gate: bfloat16 [8, 512, 1792], P('pp')
- w_up: bfloat16 [8, 512, 1792], P('pp')
- w_down: bfloat16 [8, 1792, 512], P('pp')
Outputs:
- output 1: bfloat16 [32, 512, 1792], P(('rep', 'pp')), parts along dimension 0
- output 2: bfloat16 [32, 512, 1792], P(('rep', 'pp')), parts along dimension 0
- output 3: bfloat16 [32, 1792, 512], P(('rep', 'pp')), parts along dimension 0
There are 4 independent parts. The reference program is written for one: setup_inputs(seed, part) draws one part's arguments, and reference() takes and returns one part's arrays. A program takes and returns all parts, laid end to end along the dimension named above; an argument that names none is the same for every part.
All inputs are finite; a program needn't handle non-finite values.
Results may differ from the reference program's by a relative error of at most 0.029.
Values are sent between devices in bfloat16 or wider.
A program may use at most 2 GiB of HBM per device.

```python
import jax
import jax.numpy as jnp
from jax import lax

MICRO = 16
TOKENS = 512
D = 512
FF = 1792
LAYERS = 8
NAMES = ("w_gate", "w_up", "w_down")
SHAPES = {"w_gate": (LAYERS, D, FF), "w_up": (LAYERS, D, FF), "w_down": (LAYERS, FF, D)}


def bump(key, n, height):
    away = (jnp.arange(n, dtype=jnp.int32) - jax.random.randint(key, (), 0, n, jnp.int32)) % n
    return jnp.where(away < n // 8, height, 1.0)


def together(key, own, strength):
    shared = jax.random.normal(key, own.shape[1:], jnp.float32)
    return (own + strength * shared) * lax.rsqrt(1 + strength * strength)


def setup_inputs(seed: int = 0, part: int = 0) -> dict:
    kx, kdy, ka, kb, kz, kf, kh, kl, *kw = jax.random.split(jax.random.key(seed), 8 + len(NAMES))
    kx, kdy, ka, kb = (jax.random.fold_in(k, part) for k in (kx, kdy, ka, kb))
    shape = (MICRO, TOKENS, D)
    much_x, much_dy = jax.random.uniform(kz, (2,), jnp.float32, 0.0, 1.0)
    layers = 2.0 ** jax.random.uniform(kl, (LAYERS, 1, 1), jnp.float32, -1.0, 1.0)
    x = together(ka, jax.random.normal(kx, shape, jnp.float32), much_x) * bump(kf, D, 4.0)
    dy = together(kb, jax.random.normal(kdy, shape, jnp.float32), much_dy)
    drawn = {"x": x.astype(jnp.bfloat16), "dy": (dy * (MICRO * TOKENS) ** -0.5).astype(jnp.bfloat16)}
    for key, name in zip(kw, NAMES, strict=True):
        w = jax.random.normal(key, SHAPES[name], jnp.float32) * SHAPES[name][1] ** -0.5
        drawn[name] = (w * {"w_gate": 1.0, "w_up": bump(kh, FF, 4.0), "w_down": layers}[name]).astype(jnp.bfloat16)
    return drawn


def matmul(a, w):
    return jnp.dot(a, w, preferred_element_type=jnp.float32).astype(jnp.bfloat16)


def normed(h):
    wide = h.astype(jnp.float32)
    scale = lax.rsqrt(jnp.mean(wide**2, -1, keepdims=True) + 1e-6)
    return (wide * scale).astype(jnp.bfloat16)


def layer(h, w):
    a = normed(h)
    gate = jnp.dot(a, w["w_gate"], preferred_element_type=jnp.float32)
    up = jnp.dot(a, w["w_up"], preferred_element_type=jnp.float32)
    return h + matmul((jax.nn.silu(gate) * up).astype(jnp.bfloat16), w["w_down"])


def stack(weights, h):
    return lax.scan(lambda h, w: (layer(h, w), None), h, weights)[0]


def reference(x, dy, w_gate, w_up, w_down):
    weights = dict(zip(NAMES, (w_gate, w_up, w_down), strict=True))

    def take(so_far, one):
        h, by_y = one
        _, back = jax.vjp(lambda w: stack(w, h), weights)
        return jax.tree.map(lambda total, term: total + term.astype(jnp.float32), so_far, back(by_y)[0]), None

    none_yet = {name: jnp.zeros(w.shape, jnp.float32) for name, w in weights.items()}
    by_weights, _ = lax.scan(take, none_yet, (x, dy))
    return tuple(by_weights[name].astype(jnp.bfloat16) for name in NAMES)
```

```python
import functools

import jax
import jax.numpy as jnp
from jax import lax
from jax.experimental import pallas as pl
from jax.experimental.pallas import tpu as pltpu
from jax.sharding import PartitionSpec as P

MESH = pl.DeviceIdType.MESH
BF, F32 = jnp.bfloat16, jnp.float32
STAGES = 8
AHEAD = (24, 20, 17, 14, 10, 7, 4, 0)
LATE = 1
RING = 4


def dot(a, b):
    return jnp.dot(a, b, preferred_element_type=F32)


def dot_t(a, b):
    return lax.dot_general(a, b, (((1,), (1,)), ((), ())), preferred_element_type=F32)


def norm_of(h):
    wide = h.astype(F32)
    scale = lax.rsqrt(jnp.mean(wide * wide, -1, keepdims=True) + 1e-6)
    return wide, scale, (wide * scale).astype(BF)


def kernel(
    chunk, tile, x_ref, dy_ref, wg_ref, wu_ref, wd_ref, og_ref, ou_ref, od_ref, gu_hbm,
    wg, wu, wd, acc, hst, dst, gu, hid, wst, a_t, dy_t, fout, bout,
    wsem, frecv, brecv, fsend, bsend, gout, gin, osem,
):
    s = lax.axis_index("pp")
    last = STAGES - 1
    micro, tokens, d = x_ref.shape
    ff = wg.shape[1]
    per = tokens // chunk
    chunks = micro * per
    tiles = ff // tile
    ahead = sum(jnp.where(s == i, n, 0) for i, n in enumerate(AHEAD))

    def part(ref, c):
        return ref.at[c // per, pl.ds(lax.rem(c, per) * chunk, chunk)]

    def got_f(c):
        return pltpu.make_async_copy(part(x_ref, c), hst.at[c], frecv.at[c])

    def got_b(c):
        return pltpu.make_async_copy(part(dy_ref, c), dst.at[c], brecv.at[c])

    def send_f(c):
        slot = lax.rem(c, RING)
        return pltpu.make_async_remote_copy(
            fout.at[slot], hst.at[c], fsend.at[slot], frecv.at[c], device_id={"pp": s + 1}, device_id_type=MESH
        )

    def send_b(c):
        slot = lax.rem(c, RING)
        return pltpu.make_async_remote_copy(
            bout.at[slot], dst.at[c], bsend.at[slot], brecv.at[c], device_id={"pp": s - 1}, device_id_type=MESH
        )

    def put_gu(c):
        slot = lax.rem(c, 2)
        return pltpu.make_async_copy(gu.at[slot], gu_hbm.at[c], gout.at[slot])

    def get_gu(c):
        slot = lax.rem(c, 2)
        return pltpu.make_async_copy(gu_hbm.at[c], gu.at[slot + 2], gin.at[slot])

    loads = [
        pltpu.make_async_copy(src.at[0], dst_, wsem.at[i])
        for i, (src, dst_) in enumerate(((wg_ref, wg), (wu_ref, wu), (wd_ref, wd)))
    ]

    @pl.when(s == 0)
    def _():
        got_f(0).start()

    for copy in loads:
        copy.start()

    barrier = pltpu.get_barrier_semaphore()
    for by in (1, STAGES - 1):
        pl.semaphore_signal(barrier, inc=1, device_id={"pp": lax.rem(s + by, STAGES)}, device_id_type=MESH)

    @pl.when(s == 0)
    def _():
        @pl.loop(1, chunks)
        def _(c):
            got_f(c).start()

    @pl.when(s == last)
    def _():
        @pl.loop(0, chunks)
        def _(c):
            got_b(c).start()

    def clear():
        @pl.loop(0, 3 * (d // 32))
        def _(i):
            j, r = i // (d // 32), lax.rem(i, d // 32)
            acc[j, pl.ds(r * 32, 32), :] = jnp.zeros((32, ff), F32)

    pl.when(s > 0)(clear)
    pl.semaphore_wait(barrier, 2)
    for copy in loads:
        copy.wait()

    def gate_up(c, slot, keep_hid):
        _, _, a = norm_of(hst[c])
        for n in range(tiles):
            cols = slice(n * tile, (n + 1) * tile)
            g, u = dot(a, wg[:, cols]), dot(a, wu[:, cols])
            gu[slot, 0, :, cols] = g
            gu[slot, 1, :, cols] = u
            if keep_hid:
                hid[:, cols] = (g * jax.nn.sigmoid(g) * u).astype(BF)

    def forward(c):
        slot = lax.rem(c, 2)
        got_f(c).wait()

        @pl.when(s == last)
        def _():
            gate_up(c, slot, False)

        @pl.when(s < last)
        def _():
            out = lax.rem(c, RING)

            @pl.when(c >= RING)
            def _():
                send_f(c - RING).wait_send()

            gate_up(c, slot, True)
            y = dot(hid[...], wd[...]).astype(BF)
            fout[out] = (hst[c].astype(F32) + y.astype(F32)).astype(BF)
            send_f(c).start()
            put_gu(c).start()

    def inner(c, slot, w_slot, rows):
        dy = dst[c]
        dy_t[w_slot, :, rows] = dy.T
        for n in range(tiles):
            cols = slice(n * tile, (n + 1) * tile)
            dh = dot_t(dy, wd[cols, :]).astype(BF).astype(F32)
            g, u = gu[slot, 0, :, cols], gu[slot, 1, :, cols]
            sig = jax.nn.sigmoid(g)
            silu = g * sig
            wst[w_slot, 2, rows, cols] = (silu * u).astype(BF)
            wst[w_slot, 1, rows, cols] = (dh * silu).astype(BF)
            wst[w_slot, 0, rows, cols] = (dh * u * (sig + silu * (1.0 - sig))).astype(BF)

    def backward(c):
        m = c // per
        w_slot = lax.rem(m, LATE + 1)
        slot = jnp.where(s == last, lax.rem(c, 2), lax.rem(c, 2) + 2)
        got_b(c).wait()

        @pl.when(s < last)
        def _():
            get_gu(c).wait()

        for half in range(per):
            rows = slice(half * chunk, (half + 1) * chunk)

            @pl.when((s == 0) & (lax.rem(c, per) == half))
            def _():
                a_t[w_slot, :, rows] = norm_of(hst[c])[2].T
                inner(c, slot, w_slot, rows)

            @pl.when((s > 0) & (lax.rem(c, per) == half))
            def _():
                out = lax.rem(c, RING)

                @pl.when(c >= RING)
                def _():
                    send_b(c - RING).wait_send()

                wide, scale, a = norm_of(hst[c])
                a_t[w_slot, :, rows] = a.T
                inner(c, slot, w_slot, rows)
                da = dot_t(wst[w_slot, 0, rows, :], wg[...]).astype(BF).astype(F32)
                da = (da + dot_t(wst[w_slot, 1, rows, :], wu[...]).astype(BF).astype(F32)).astype(BF).astype(F32)
                inner_sum = jnp.sum(da * wide, -1, keepdims=True) * (1.0 / d)
                dwide = scale * da - wide * (scale * scale * scale * inner_sum)
                bout[out] = (dst[c].astype(F32) + dwide.astype(BF).astype(F32)).astype(BF)
                send_b(c).start()

    def weights(m):
        slot = lax.rem(m, LATE + 1)
        for j in range(3):
            for n in range(tiles):
                cols = slice(n * tile, (n + 1) * tile)
                lhs = dy_t[slot] if j == 2 else a_t[slot]
                term = dot(lhs, wst[slot, j, :, cols]).astype(BF).astype(F32)
                acc[j, :, cols] = acc[j, :, cols] + term

    @pl.loop(0, chunks + max(AHEAD) + per * LATE)
    def _(t):
        @pl.when((s < last) & (t >= 2) & (t < chunks + 2))
        def _():
            put_gu(t - 2).wait()

        @pl.when(t < chunks)
        def _():
            forward(t)

        soon = t - ahead + 1

        @pl.when((s < last) & (soon >= 0) & (soon < chunks))
        def _():
            get_gu(soon).start()

        back = t - ahead
        pl.when((s == 0) & (back == 0))(clear)

        @pl.when((back >= 0) & (back < chunks))
        def _():
            backward(back)

        m = (back + 1) // per - 1 - LATE

        @pl.when((lax.rem(back + 1, per) == 0) & (back + 1 > per * LATE) & (m < micro))
        def _():
            weights(m)

    @pl.when(s < last)
    def _():
        @pl.loop(chunks - RING, chunks)
        def _(c):
            send_f(c).wait_send()

    @pl.when(s > 0)
    def _():
        @pl.loop(chunks - RING, chunks)
        def _(c):
            send_b(c).wait_send()

    copies = []
    for j, ref in enumerate((og_ref, ou_ref, od_ref)):
        for n in range(tiles):
            cols = slice(n * tile, (n + 1) * tile)
            wst[0, j, :, cols] = acc[j, :, cols].astype(BF)
        copies.append(pltpu.make_async_copy(wst.at[0, j], ref.at[0], osem.at[j]))
        copies[-1].start()
    for copy in copies:
        copy.wait()


def solution(mesh):
    def step(x, dy, w_gate, w_up, w_down):
        micro, tokens, d = x.shape
        ff = w_gate.shape[2]
        chunk, tile = tokens // 2, 256
        chunks = 2 * micro
        any_, vmem = pl.BlockSpec(memory_space=pl.ANY), pltpu.VMEM
        dma = pltpu.SemaphoreType.DMA
        flat = jax.ShapeDtypeStruct((1, d, ff), BF)
        by_gate, by_up, by_down, _ = pl.pallas_call(
            functools.partial(kernel, chunk, tile),
            name="stages",
            out_shape=(flat, flat, flat, jax.ShapeDtypeStruct((chunks, 2, chunk, ff), F32)),
            in_specs=[any_] * 5,
            out_specs=(any_,) * 4,
            scratch_shapes=[
                vmem((d, ff), BF),
                vmem((d, ff), BF),
                vmem((ff, d), BF),
                vmem((3, d, ff), F32),
                vmem((chunks, chunk, d), BF),
                vmem((chunks, chunk, d), BF),
                vmem((4, 2, chunk, ff), F32),
                vmem((chunk, ff), BF),
                vmem((LATE + 1, 3, tokens, ff), BF),
                vmem((LATE + 1, d, tokens), BF),
                vmem((LATE + 1, d, tokens), BF),
                vmem((RING, chunk, d), BF),
                vmem((RING, chunk, d), BF),
                dma((3,)),
                dma((chunks,)),
                dma((chunks,)),
                dma((RING,)),
                dma((RING,)),
                dma((2,)),
                dma((2,)),
                dma((3,)),
            ],
            compiler_params=pltpu.CompilerParams(
                collective_id=0, has_side_effects=True, vmem_limit_bytes=67043328
            ),
        )(x, dy, w_gate, w_up, w_down)
        return by_gate, by_up, jnp.swapaxes(by_down, 1, 2)

    return jax.shard_map(
        step,
        mesh=mesh,
        in_specs=(P("rep", None, None),) * 2 + (P("pp", None, None),) * 3,
        out_specs=(P(("rep", "pp"), None, None),) * 3,
        check_vma=False,
    )
```

```python
import functools

import jax
import jax.numpy as jnp
from jax import lax
from jax.experimental import pallas as pl
from jax.experimental.pallas import tpu as pltpu
from jax.sharding import PartitionSpec as P

MESH = pl.DeviceIdType.MESH
BF, F32 = jnp.bfloat16, jnp.float32
STAGES = 8
LANES = 128
AHEAD = (31, 27, 19, 16, 11, 8, 3, 0)
NEAR = 4
LATE = (2, 2, 4, 5, 7, 8, 11, 12)
RING = 4


def dot(a, b):
    return jnp.dot(a, b, preferred_element_type=F32)


def dot_t(a, b):
    return lax.dot_general(a, b, (((1,), (1,)), ((), ())), preferred_element_type=F32)


def kernel(
    chunk, tile, x_ref, dy_ref, wg_ref, wu_ref, wd_ref, og_ref, ou_ref, od_ref, gu_hbm, w_hbm,
    wg, wu, wd, acc, hst, dst, gu, hid, dgu, win, cur, abuf, fbuf, sbuf, fout, bout,
    wsem, frecv, brecv, fsend, bsend, gout, gin, hout, dout, wsin, osem,
):
    s = lax.axis_index("pp")
    last = STAGES - 1
    micro, tokens, d = x_ref.shape
    ff = wg.shape[1]
    per = tokens // chunk
    chunks = micro * per
    tiles = ff // tile
    ahead = sum(jnp.where(s == i, n, 0) for i, n in enumerate(AHEAD))
    late = sum(jnp.where(s == i, n, 0) for i, n in enumerate(LATE))
    near = ahead < NEAR
    strip = min(chunk, 64)
    strips = [slice(r, r + strip) for r in range(0, chunk, strip)]
    blocks = d // chunk

    def part(ref, c):
        return ref.at[c // per, pl.ds(lax.rem(c, per) * chunk, chunk)]

    def got_f(c):
        return pltpu.make_async_copy(part(x_ref, c), hst.at[c], frecv.at[c])

    def got_b(c):
        return pltpu.make_async_copy(part(dy_ref, c), dst.at[c], brecv.at[c])

    def send_f(c):
        slot = lax.rem(c, RING)
        return pltpu.make_async_remote_copy(
            fout.at[slot], hst.at[c], fsend.at[slot], frecv.at[c], device_id={"pp": s + 1}, device_id_type=MESH
        )

    def send_b(c):
        slot = lax.rem(c, RING)
        return pltpu.make_async_remote_copy(
            bout.at[slot], dst.at[c], bsend.at[slot], brecv.at[c], device_id={"pp": s - 1}, device_id_type=MESH
        )

    def put_gu(c):
        slot = lax.rem(c, 2)
        return pltpu.make_async_copy(gu.at[slot], gu_hbm.at[c], gout.at[slot])

    def get_gu(c):
        slot = lax.rem(c, 2)
        return pltpu.make_async_copy(gu_hbm.at[c], gu.at[slot + 2], gin.at[slot])

    def put_hid(c):
        slot = lax.rem(c, 2)
        to = w_hbm.at[c // per, 2, pl.ds(lax.rem(c, per) * chunk, chunk)]
        return pltpu.make_async_copy(hid.at[slot], to, hout.at[slot])

    def put_dgu(c):
        slot = lax.rem(c, 2)
        to = w_hbm.at[c // per, pl.ds(0, 2), pl.ds(lax.rem(c, per) * chunk, chunk)]
        return pltpu.make_async_copy(dgu.at[slot], to, dout.at[slot])

    def get_w(m):
        return pltpu.make_async_copy(w_hbm.at[m], win, wsin)

    loads = [
        pltpu.make_async_copy(src.at[0], dst_, wsem.at[i])
        for i, (src, dst_) in enumerate(((wg_ref, wg), (wu_ref, wu), (wd_ref, wd)))
    ]

    @pl.when(s == 0)
    def _():
        got_f(0).start()

    for copy in loads:
        copy.start()

    barrier = pltpu.get_barrier_semaphore()
    for by in (1, STAGES - 1):
        pl.semaphore_signal(barrier, inc=1, device_id={"pp": lax.rem(s + by, STAGES)}, device_id_type=MESH)

    @pl.when(s == 0)
    def _():
        @pl.loop(1, chunks)
        def _(c):
            got_f(c).start()

    @pl.when(s == last)
    def _():
        @pl.loop(0, chunks)
        def _(c):
            got_b(c).start()

    def clear():
        @pl.loop(0, 3 * (d // 32))
        def _(i):
            j, r = i // (d // 32), lax.rem(i, d // 32)
            acc[j, pl.ds(r * 32, 32), :] = jnp.zeros((32, ff), F32)

    pl.when(s > 0)(clear)
    pl.semaphore_wait(barrier, 2)
    for copy in loads:
        copy.wait()

    def norm(h, to, sbuf=None):
        for rows in strips:
            wide = h[rows, :].astype(F32)
            scale = lax.rsqrt(jnp.mean(wide * wide, -1, keepdims=True) + 1e-6)
            if sbuf is not None:
                sbuf[rows, :] = jnp.broadcast_to(scale, (strip, LANES))
            to[rows, :] = (wide * scale).astype(BF)

    def gate_up(c, slot):
        norm(hst[c], fbuf)
        h_slot = lax.rem(c, 2)
        a = fbuf[...]
        for n in range(tiles):
            cols = slice(n * tile, (n + 1) * tile)
            g, u = dot(a, wg[:, cols]), dot(a, wu[:, cols])
            sig = jax.nn.sigmoid(g)
            silu = g * sig
            gu[slot, 0, :, cols] = u * (sig + silu * (1.0 - sig))
            gu[slot, 1, :, cols] = silu
            hid[h_slot, :, cols] = (silu * u).astype(BF)

    def down(c, out):
        y = dot(hid[lax.rem(c, 2)], wd[...]).astype(BF)
        fout[out] = (hst[c].astype(F32) + y.astype(F32)).astype(BF)

    def forward(c):
        slot = jnp.where(near, lax.rem(c, 4), lax.rem(c, 2))
        got_f(c).wait()

        @pl.when(s == last)
        def _():
            gate_up(c, slot)

        @pl.when(s < last)
        def _():
            out = lax.rem(c, RING)

            @pl.when(c >= RING)
            def _():
                send_f(c - RING).wait_send()

            gate_up(c, slot)
            down(c, out)
            send_f(c).start()

        put_hid(c).start()

        @pl.when(jnp.logical_not(near))
        def _():
            put_gu(c).start()

    def turn(ref, c, value):
        t = value.T
        for i in range(blocks):
            ref[c, :, i * chunk : (i + 1) * chunk] = t[i * chunk : (i + 1) * chunk, :]

    def inner(c, slot, to):
        dy = cur[1]
        for n in range(tiles):
            cols = slice(n * tile, (n + 1) * tile)
            dh = dot_t(dy, wd[cols, :]).astype(BF).astype(F32)
            dgu[to, 0, :, cols] = (dh * gu[slot, 0, :, cols]).astype(BF)
            dgu[to, 1, :, cols] = (dh * gu[slot, 1, :, cols]).astype(BF)

    def back_to_hidden(c, slot, to):
        cur[0] = hst[c]
        cur[1] = dst[c]
        norm(cur[0], abuf, sbuf)
        inner(c, slot, to)
        turn(dst, c, cur[1])
        turn(hst, c, abuf[...])

    def back_to_states(to, out):
        da0 = dot_t(dgu[to, 0], wg[...]).astype(BF).astype(F32)
        da1 = dot_t(dgu[to, 1], wu[...]).astype(BF).astype(F32)
        for rows in strips:
            da = (da0[rows, :] + da1[rows, :]).astype(BF).astype(F32)
            wide = cur[0, rows, :].astype(F32)
            scale = jnp.concatenate([sbuf[rows, :]] * (d // LANES), axis=1)
            inner_sum = jnp.sum(da * wide, -1, keepdims=True) * (1.0 / d)
            dwide = scale * da - wide * (scale * scale * scale * inner_sum)
            bout[out, rows, :] = (cur[1, rows, :].astype(F32) + dwide.astype(BF).astype(F32)).astype(BF)

    def both_ways(c, b):
        out_f, out_b, to = lax.rem(c, RING), lax.rem(b, RING), lax.rem(b, 2)
        f_slot = jnp.where(near, lax.rem(c, 4), lax.rem(c, 2))
        b_slot = jnp.where(near, lax.rem(b, 4), lax.rem(b, 2) + 2)
        got_f(c).wait()
        got_b(b).wait()

        @pl.when(jnp.logical_not(near))
        def _():
            get_gu(b).wait()

        @pl.when(c >= RING)
        def _():
            send_f(c - RING).wait_send()

        @pl.when(b >= RING)
        def _():
            send_b(b - RING).wait_send()

        back_to_hidden(b, b_slot, to)
        gate_up(c, f_slot)
        back_to_states(to, out_b)
        down(c, out_f)
        send_b(b).start()
        send_f(c).start()
        put_hid(c).start()
        put_dgu(b).start()

        @pl.when(jnp.logical_not(near))
        def _():
            put_gu(c).start()

    def backward(c):
        to = lax.rem(c, 2)
        slot = jnp.where(near, lax.rem(c, 4), lax.rem(c, 2) + 2)
        got_b(c).wait()

        @pl.when(jnp.logical_not(near))
        def _():
            get_gu(c).wait()

        @pl.when(s == 0)
        def _():
            cur[1] = dst[c]
            norm(hst[c], abuf)
            inner(c, slot, to)
            turn(dst, c, cur[1])
            turn(hst, c, abuf[...])

        @pl.when(s > 0)
        def _():
            out = lax.rem(c, RING)

            @pl.when(c >= RING)
            def _():
                send_b(c - RING).wait_send()

            back_to_hidden(c, slot, to)
            back_to_states(to, out)
            send_b(c).start()

        put_dgu(c).start()

    def weights(m):
        get_w(m).wait()
        for j, ref in ((2, dst), (0, hst), (1, hst)):
            lhs = [
                jnp.concatenate([ref[m * per + k, :, i * chunk : (i + 1) * chunk] for i in range(blocks)], axis=0)
                for k in range(per)
            ]
            for n in range(tiles):
                cols = slice(n * tile, (n + 1) * tile)
                term = sum(dot(lhs[k], win[j, k * chunk : (k + 1) * chunk, cols]) for k in range(per))
                acc[j, :, cols] = acc[j, :, cols] + term.astype(BF).astype(F32)

    @pl.loop(0, chunks + max(n + per * l for n, l in zip(AHEAD, LATE)))
    def _(t):
        @pl.when((t >= 2) & (t < chunks + 2))
        def _():
            put_hid(t - 2).wait()

            @pl.when(jnp.logical_not(near))
            def _():
                put_gu(t - 2).wait()

        soon, back = t - ahead + 2, t - ahead

        @pl.when((back >= 2) & (back < chunks + 2))
        def _():
            put_dgu(back - 2).wait()

        m = (back + 1) // per - 1 - late
        due = (lax.rem(back + 1, per) == 0) & (back + 1 > per * late) & (m < micro)

        early = back // per - late

        @pl.when((lax.rem(back, per) == 0) & (back >= per * late) & (early < micro))
        def _():
            get_w(early).start()

        both = (s > 0) & (s < last) & (t < chunks) & (back >= 0)
        pl.when(both)(lambda: both_ways(t, back))
        alone = jnp.logical_not(both)
        pl.when(alone & (t < chunks))(lambda: forward(t))
        pl.when((s == 0) & (back == 0))(clear)
        pl.when(alone & (back >= 0) & (back < chunks))(lambda: backward(back))

        @pl.when(jnp.logical_not(near) & (soon >= 0) & (soon < chunks))
        def _():
            get_gu(soon).start()

        @pl.when(due)
        def _():
            weights(m)

    @pl.when(s < last)
    def _():
        @pl.loop(chunks - RING, chunks)
        def _(c):
            send_f(c).wait_send()

    @pl.when(s > 0)
    def _():
        @pl.loop(chunks - RING, chunks)
        def _(c):
            send_b(c).wait_send()

    copies = []
    for j, ref in enumerate((og_ref, ou_ref, od_ref)):
        for n in range(tiles):
            cols = slice(n * tile, (n + 1) * tile)
            win[j, :, cols] = acc[j, :, cols].astype(BF)
        copies.append(pltpu.make_async_copy(win.at[j], ref.at[0], osem.at[j]))
        copies[-1].start()
    for copy in copies:
        copy.wait()


def solution(mesh):
    def step(x, dy, w_gate, w_up, w_down):
        micro, tokens, d = x.shape
        ff = w_gate.shape[2]
        chunk, tile = tokens // 2, 256
        chunks = 2 * micro
        any_, vmem = pl.BlockSpec(memory_space=pl.ANY), pltpu.VMEM
        dma = pltpu.SemaphoreType.DMA
        flat = jax.ShapeDtypeStruct((1, d, ff), BF)
        by_gate, by_up, by_down, _, _ = pl.pallas_call(
            functools.partial(kernel, chunk, tile),
            name="stages",
            out_shape=(
                flat,
                flat,
                flat,
                jax.ShapeDtypeStruct((chunks, 2, chunk, ff), F32),
                jax.ShapeDtypeStruct((micro, 3, tokens, ff), BF),
            ),
            in_specs=[any_] * 5,
            out_specs=(any_,) * 5,
            scratch_shapes=[
                vmem((d, ff), BF),
                vmem((d, ff), BF),
                vmem((ff, d), BF),
                vmem((3, d, ff), F32),
                vmem((chunks, chunk, d), BF),
                vmem((chunks, chunk, d), BF),
                vmem((4, 2, chunk, ff), F32),
                vmem((2, chunk, ff), BF),
                vmem((2, 2, chunk, ff), BF),
                vmem((3, tokens, ff), BF),
                vmem((2, chunk, d), BF),
                vmem((chunk, d), BF),
                vmem((chunk, d), BF),
                vmem((chunk, LANES), F32),
                vmem((RING, chunk, d), BF),
                vmem((RING, chunk, d), BF),
                dma((3,)),
                dma((chunks,)),
                dma((chunks,)),
                dma((RING,)),
                dma((RING,)),
                dma((2,)),
                dma((2,)),
                dma((2,)),
                dma((2,)),
                dma,
                dma((3,)),
            ],
            compiler_params=pltpu.CompilerParams(
                collective_id=0, has_side_effects=True, vmem_limit_bytes=67043328
            ),
        )(x, dy, w_gate, w_up, w_down)
        return by_gate, by_up, jnp.swapaxes(by_down, 1, 2)

    return jax.shard_map(
        step,
        mesh=mesh,
        in_specs=(P("rep", None, None),) * 2 + (P("pp", None, None),) * 3,
        out_specs=(P(("rep", "pp"), None, None),) * 3,
        check_vma=False,
    )
```
